32 devices in a mesh: groups: 2 (over y), tensor: 4 (over z), dp: 2 (over x), seq: 2 (over core).
Axes of the slice: x: 2, y: 2, z: 4, core: 2. Of those that a mesh axis runs over, the one named last changes fastest.
Arguments:
- attn_heads: bfloat16 [256, 8192], P(('groups', 'dp', 'seq'), 'tensor'), parts along dimension 0, may hold values from -6 to 6
- out_weight: bfloat16 [8192, 8192], P(('tensor', 'seq')), may hold values from -0.09375 to 0.09375
- residual: bfloat16 [256, 8192], P(('groups', 'dp', 'seq'), 'tensor'), parts along dimension 0, may hold values from -32 to 32
- norm_gain: bfloat16 [8192], P('tensor'), may hold values from 0.099609375 to 1.8984375
Outputs:
- stream: bfloat16 [256, 8192], P(('groups', 'dp', 'seq'), 'tensor'), parts along dimension 0
- normed: bfloat16 [256, 8192], P(('groups', 'dp', 'seq')), parts along dimension 0
The draws below stay inside these ranges and needn't reach their ends.
There are 2 independent parts, one for each index of `groups`. The reference program is written for one: setup_inputs(seed, part) draws one part's arguments, and reference() takes and returns one part's arrays. A program takes and returns all parts, laid end to end along the dimension named above; an argument that names none is the same for every part. Nothing has to cross between parts.
All inputs are finite; a program needn't handle non-finite values.
Results may differ from the reference program's by a relative error of at most 0.0056.
Values may be sent and summed in bfloat16 or wider, within the bound.
No kernel may reach another device: no remote copies, remote signals or barrier semaphores. Data moves between devices by JAX's collectives and lax.ppermute only.
A program may use at most 64 MiB of HBM per device.

```python
import math
import jax
import jax.numpy as jnp
from jax import lax

D = 8192
BATCH = 128


def draw_residual(key, part):
    key = jax.random.fold_in(key, 7)
    k_row, k_col, k_base = jax.random.split(key, 3)
    row_scale = jnp.exp(jax.random.uniform(k_row, (BATCH, 1), jnp.float32, math.log(0.2), math.log(2.0)))
    ramp = 1.0 + 0.8 * jnp.arange(D, dtype=jnp.float32) / D
    col_scale = ramp[None, :] * jnp.exp(jax.random.uniform(k_col, (1, D), jnp.float32, math.log(0.4), math.log(2.2)))
    base = jax.random.normal(k_base, (BATCH, D), jnp.float32)
    return jnp.clip(row_scale * col_scale * base, -32.0, 32.0).astype(jnp.bfloat16)


def with_spikes(values, rng, source, target, shards_of, factor):
    def block_of(dim):
        return (jnp.arange(values.shape[dim]) // (values.shape[dim] // shards_of)).reshape((-1,) + (1,) * (values.ndim - 1 - dim))

    near = jax.random.permutation(rng, shards_of)[block_of(target)]
    second = (block_of(target) + shards_of // 2) % shards_of
    return jnp.where((block_of(source) == near) | (block_of(source) == second), factor * values, values)


def shard_levels(rng, extent, cuts, low, largest):
    def one(axis_at, blocks):
        draws = jax.random.uniform(jax.random.fold_in(jax.random.fold_in(rng, 6), axis_at), (blocks,), jnp.float32, low / len(cuts), largest / len(cuts))
        return jnp.repeat(jnp.exp(draws), extent[axis_at] // blocks).reshape((-1,) + (1,) * (len(extent) - axis_at - 1))

    level = one(*cuts[0])
    for cut in cuts[1:]:
        level = level * one(*cut)
    return level


def gaussian(key, dims, scale, reach, shards=(), held_as=jnp.bfloat16):
    entries = jax.random.normal(key, dims, jnp.float32) * scale
    if len(shards) > 0:
        entries = shard_levels(key, dims, shards, -0.22, 0.18) * entries
    return jnp.clip(entries, min=-reach, max=reach).astype(held_as)


def heavy_noise(rng, dims, scale, bound, cuts, heavy, kind=jnp.bfloat16):
    result = scale * jax.random.normal(rng, dims, jnp.float32)
    if cuts:
        result = result * shard_levels(rng, dims, cuts, -0.22, 0.18)
    return jnp.clip(with_spikes(result, jax.random.fold_in(rng, 3), *heavy), -bound, bound).astype(kind)


def setup_inputs(seed: int = 0, part: int = 0) -> dict:
    keys = jax.random.split(jax.random.key(seed), 5)
    part_splits = jax.random.split(jax.random.fold_in(keys[4], part), 5)
    return {
        "attn_heads": gaussian(part_splits[0], (BATCH, D), 1.0, 6.0, ((0, 4), (1, 4))),
        "out_weight": heavy_noise(keys[1], (D, D), D ** -0.5, 0.09375, ((0, 8),), (0, 1, 8, 2.0)),
        "residual": draw_residual(jax.random.fold_in(jax.random.fold_in(keys[4], part), 71), part),
        "norm_gain": jnp.clip(1.0 + 0.18 * jax.random.normal(keys[3], (D,), jnp.float32), 0.099609375, 1.8984375).astype(jnp.bfloat16),
    }


def reference(attn_heads, out_weight, residual, norm_gain):
    attended = jnp.dot(attn_heads, out_weight, preferred_element_type=jnp.float32)
    stream = (residual.astype(jnp.float32) + attended).astype(jnp.bfloat16)
    stream_float = stream.astype(jnp.float32)
    mean_square = lax.optimization_barrier(jnp.mean(stream_float * stream_float, axis=1, keepdims=True))
    normed = stream_float * lax.rsqrt(mean_square + 1e-05) * norm_gain.astype(jnp.float32)[None, :]
    return (stream, normed.astype(jnp.bfloat16))
```

```python
import functools

import jax
import jax.numpy as jnp
from jax import lax
from jax.experimental import pallas as pl
from jax.experimental.pallas import tpu as pltpu
from jax.sharding import PartitionSpec as P

VMEM = pltpu.VMEM
HBM = pltpu.HBM
MIB = 1024 * 1024
F32, BF16 = jnp.float32, jnp.bfloat16


def project_kernel(tensor, chunk, own_ref, peer_ref, weight, keep_ref, give_ref, held, sems):
    depth, width = weight.shape
    block = width // tensor
    per_block = block // chunk
    rank = lax.axis_index("tensor")
    half = lax.axis_index("seq")

    def copy(index):
        step, piece = divmod(index, per_block)
        start = (rank ^ step) * block + piece * chunk
        return pltpu.make_async_copy(
            weight.at[:, pl.ds(pl.multiple_of(start, 128), chunk)], held.at[index], sems.at[index]
        )

    count = tensor * per_block
    for index in range(count):
        copy(index).start()
    features = pl.ds(pl.multiple_of(half * depth, 128), depth)
    rows = own_ref.shape[0]
    operand = jnp.concatenate([own_ref[:, features], peer_ref[:, features]], axis=0)
    for index in range(count):
        step, piece = divmod(index, per_block)
        copy(index).wait()
        product = jnp.dot(operand, held[index], preferred_element_type=F32)
        columns = pl.ds(piece * chunk, chunk)
        keep_ref[step, :, columns] = product[:rows]
        give_ref[step, :, columns] = product[rows:].astype(BF16)


def project(own, peer, weight, tensor):
    rows = own.shape[0]
    depth, width = weight.shape
    block = width // tensor
    chunk = min(block, 512)
    count = width // chunk
    return pl.pallas_call(
        functools.partial(project_kernel, tensor, chunk),
        in_specs=[
            pl.BlockSpec(memory_space=VMEM),
            pl.BlockSpec(memory_space=VMEM),
            pl.BlockSpec(memory_space=HBM),
        ],
        out_specs=[pl.BlockSpec(memory_space=VMEM)] * 2,
        out_shape=[
            jax.ShapeDtypeStruct((tensor, rows, block), F32),
            jax.ShapeDtypeStruct((tensor, rows, block), BF16),
        ],
        scratch_shapes=[
            VMEM((count, depth, chunk), BF16),
            pltpu.SemaphoreType.DMA((count,)),
        ],
        compiler_params=pltpu.CompilerParams(vmem_limit_bytes=2 * weight.size + 8 * MIB),
        name="project",
    )(own, peer, pltpu.with_memory_space_constraint(weight, HBM))


def pair_kernel(keep_ref, got_ref, residual_ref, base_ref, *send_refs):
    base_ref[...] = residual_ref[...].astype(F32) + keep_ref[0] + got_ref[0].astype(F32)
    for step, send_ref in enumerate(send_refs, 1):
        send_ref[...] = (keep_ref[step] + got_ref[step].astype(F32)).astype(BF16)


def pair_sum(keep, got, residual):
    tensor, rows, block = keep.shape
    return pl.pallas_call(
        pair_kernel,
        in_specs=[pl.BlockSpec(memory_space=VMEM)] * 3,
        out_specs=[pl.BlockSpec(memory_space=VMEM)] * tensor,
        out_shape=[jax.ShapeDtypeStruct((rows, block), F32)]
        + [jax.ShapeDtypeStruct((rows, block), BF16)] * (tensor - 1),
        compiler_params=pltpu.CompilerParams(vmem_limit_bytes=6 * MIB),
        name="pair_sum",
    )(keep, got, residual)


def stream_kernel(base_ref, *refs):
    total = base_ref[...]
    for ref in refs[:-2]:
        total = total + ref[...].astype(F32)
    stream = total.astype(BF16)
    refs[-2][...] = stream
    refs[-1][...] = stream


def finish_stream(base, parts):
    return pl.pallas_call(
        stream_kernel,
        in_specs=[pl.BlockSpec(memory_space=VMEM)] * (1 + len(parts)),
        out_specs=[pl.BlockSpec(memory_space=VMEM)] * 2,
        out_shape=[jax.ShapeDtypeStruct(base.shape, BF16)] * 2,
        compiler_params=pltpu.CompilerParams(vmem_limit_bytes=6 * MIB),
        name="finish_stream",
    )(base, *parts)


def norm_kernel(tensor, *refs):
    pieces, gains, out_ref = refs[:tensor], refs[tensor : 2 * tensor], refs[-1]
    block = pieces[0].shape[1]
    rank = lax.axis_index("tensor")
    total = 0.0
    for piece in pieces:
        value = piece[...].astype(F32)
        total = total + jnp.sum(value * value, axis=1, keepdims=True)
    scale = lax.rsqrt(total / (tensor * block) + 1e-05)
    for step in range(tensor):
        start = pl.multiple_of((rank ^ step) * block, 128)
        value = pieces[step][...].astype(F32) * scale * gains[step][...].astype(F32)
        out_ref[:, pl.ds(start, block)] = value.astype(BF16)


def normalize(pieces, gains):
    tensor = len(pieces)
    rows, block = pieces[0].shape
    return pl.pallas_call(
        functools.partial(norm_kernel, tensor),
        in_specs=[pl.BlockSpec(memory_space=VMEM)] * (2 * tensor),
        out_specs=pl.BlockSpec(memory_space=VMEM),
        out_shape=jax.ShapeDtypeStruct((rows, tensor * block), BF16),
        compiler_params=pltpu.CompilerParams(vmem_limit_bytes=6 * MIB),
        name="normalize",
    )(*pieces, *gains)


def on_device(attn_heads, out_weight, residual, norm_gain):
    tensor = lax.axis_size("tensor")
    swap = [(0, 1), (1, 0)]

    def exchange(value, step):
        return lax.ppermute(value, "tensor", [(i, i ^ step) for i in range(tensor)])

    peer = lax.ppermute(attn_heads, "seq", swap)
    keep, give = project(attn_heads, peer, out_weight, tensor)
    got = lax.ppermute(give, "seq", swap)
    base, *sends = pair_sum(keep, got, residual)
    gain = norm_gain[None, :]
    gains = [gain] + [exchange(gain, step) for step in range(1, tensor)]
    parts = [exchange(value, step) for step, value in enumerate(sends, 1)]
    stream, piece = finish_stream(base, parts)
    pieces = [piece] + [exchange(piece, step) for step in range(1, tensor)]
    return stream, normalize(pieces, gains)


def solution(mesh):
    in_specs = (
        P(("groups", "dp", "seq"), "tensor"),
        P(("tensor", "seq"), None),
        P(("groups", "dp", "seq"), "tensor"),
        P("tensor"),
    )
    out_specs = (P(("groups", "dp", "seq"), "tensor"), P(("groups", "dp", "seq"), None))
    return jax.shard_map(
        on_device, mesh=mesh, in_specs=in_specs, out_specs=out_specs, check_vma=False
    )
```

```python
import functools

import jax
import jax.numpy as jnp
from jax import lax
from jax.experimental import pallas as pl
from jax.experimental.pallas import tpu as pltpu
from jax.sharding import PartitionSpec as P


VMEM, HBM = pltpu.VMEM, pltpu.HBM
MIB = 1024 * 1024
F32, BF16 = jnp.float32, jnp.bfloat16
LANES = 128
SPLITS = 1


def call(kernel, in_specs, out_shape, limit, scratch=()):
    return pl.pallas_call(
        kernel,
        in_specs=[pl.BlockSpec(memory_space=space) for space in in_specs],
        out_specs=[pl.BlockSpec(memory_space=VMEM)] * len(out_shape),
        out_shape=out_shape,
        scratch_shapes=list(scratch),
        compiler_params=pltpu.CompilerParams(vmem_limit_bytes=limit),
    )


def project_kernel(tensor, chunk, steps, own_hbm, peer_ref, weight, keep_ref, give_ref, own_ref, held, own_sem, sems):
    depth, width = weight.shape
    block = width // tensor
    per_block = block // chunk
    rank = lax.axis_index("tensor")
    features = pl.ds(pl.multiple_of(lax.axis_index("seq") * depth, LANES), depth)
    own_copy = pltpu.make_async_copy(own_hbm.at[:, features], own_ref, own_sem)
    own_copy.start()

    def copy(index):
        place, piece = divmod(index, per_block)
        start = (rank ^ steps[place]) * block + piece * chunk
        return pltpu.make_async_copy(
            weight.at[:, pl.ds(pl.multiple_of(start, LANES), chunk)], held.at[index], sems.at[index]
        )

    count = len(steps) * per_block
    for index in range(count):
        copy(index).start()
    own_copy.wait()
    rows = own_ref.shape[0]
    operand = jnp.concatenate([own_ref[...], peer_ref[:, features]], axis=0)
    for index in range(count):
        place, piece = divmod(index, per_block)
        copy(index).wait()
        product = jnp.dot(operand, held[index], preferred_element_type=F32)
        columns = pl.ds(piece * chunk, chunk)
        keep_ref[place, :, columns] = product[:rows]
        give_ref[place, :, columns] = product[rows:].astype(BF16)


def project(own, peer, weight, tensor, steps):
    rows = own.shape[0]
    depth, width = weight.shape
    block = width // tensor
    chunk = min(block, 512)
    count = len(steps) * block // chunk
    return call(
        functools.partial(project_kernel, tensor, chunk, steps),
        [HBM, VMEM, HBM],
        [
            jax.ShapeDtypeStruct((len(steps), rows, block), F32),
            jax.ShapeDtypeStruct((len(steps), rows, block), BF16),
        ],
        2 * depth * chunk * count + 4 * MIB,
        [
            VMEM((rows, depth), BF16),
            VMEM((count, depth, chunk), BF16),
            pltpu.SemaphoreType.DMA(()),
            pltpu.SemaphoreType.DMA((count,)),
        ],
    )(
        pltpu.with_memory_space_constraint(own, HBM),
        peer,
        pltpu.with_memory_space_constraint(weight, HBM),
    )


def pair_kernel(steps, keep_ref, got_ref, residual_ref, gain_ref, *out_refs):
    _, rows, block = keep_ref.shape
    part = rows // SPLITS
    targets = iter(out_refs)
    for place, step in enumerate(steps):
        for split in range(SPLITS):
            target = next(targets)
            span = slice(split * part, (split + 1) * part)
            for tile in range(block // LANES):
                columns = slice(tile * LANES, (tile + 1) * LANES)
                value = keep_ref[place, span, columns] + got_ref[place, span, columns].astype(F32)
                if step == 0:
                    value = value + residual_ref[span, columns].astype(F32)
                target[tile * part : (tile + 1) * part, :] = value.astype(target.dtype)
            if step and not split:
                target[block // LANES * part :, :] = gain_ref[...]


def pair_sum(steps, keep, got, residual, gain):
    _, rows, block = keep.shape
    length = rows // SPLITS * block // LANES
    shapes = []
    for step in steps:
        for split in range(SPLITS):
            extra = gain.shape[0] if step and not split else 0
            shapes.append(jax.ShapeDtypeStruct((length + extra, LANES), BF16 if step else F32))
    outs = call(functools.partial(pair_kernel, steps), [VMEM] * 4, shapes, 6 * MIB)(
        keep, got, residual, gain
    )
    return {step: outs[i * SPLITS : (i + 1) * SPLITS] for i, step in enumerate(steps)}


def stream_kernel(base_ref, *refs):
    length = base_ref.shape[0]
    total = base_ref[...]
    for ref in refs[:-1]:
        total = total + ref[:length, :].astype(F32)
    refs[-1][...] = total.astype(BF16)


def finish_stream(base, parts):
    return call(
        stream_kernel, [VMEM] * (1 + len(parts)), [jax.ShapeDtypeStruct(base.shape, BF16)], 4 * MIB
    )(base, *parts)[0]


def norm_kernel(tensor, rows, block, *refs):
    pieces, refs = refs[: tensor * SPLITS], refs[tensor * SPLITS :]
    gains, (stream_ref, out_ref) = refs[:tensor], refs[tensor:]
    part = rows // SPLITS
    tiles = block // LANES
    rank = lax.axis_index("tensor")
    starts = [(rank ^ step) * block for step in range(tensor)]
    gain_rows = []
    for step, ref in enumerate(gains):
        first = tiles * part if step else 0
        gain_rows.append(ref[first:, :].astype(F32))
    for split in range(SPLITS):
        span = slice(split * part, (split + 1) * part)
        total = jnp.zeros((part, LANES), F32)
        for step in range(tensor):
            for tile in range(tiles):
                value = pieces[step * SPLITS + split][tile * part : (tile + 1) * part, :].astype(F32)
                total = total + value * value
        mean_square = jnp.sum(total, axis=1, keepdims=True) / (tensor * block)
        scale = jnp.broadcast_to(lax.rsqrt(mean_square + 1e-05), (part, LANES))
        for step in range(tensor):
            for tile in range(tiles):
                piece = pieces[step * SPLITS + split][tile * part : (tile + 1) * part, :]
                value = piece.astype(F32) * scale * gain_rows[step][tile : tile + 1, :]
                columns = pl.ds(pl.multiple_of(starts[step] + tile * LANES, LANES), LANES)
                out_ref[span, columns] = value.astype(BF16)
                if step == 0:
                    stream_ref[span, tile * LANES : (tile + 1) * LANES] = piece


def normalize(pieces, gains, rows, block):
    tensor = len(gains)
    return call(
        functools.partial(norm_kernel, tensor, rows, block),
        [VMEM] * (tensor * SPLITS + tensor),
        [
            jax.ShapeDtypeStruct((rows, block), BF16),
            jax.ShapeDtypeStruct((rows, tensor * block), BF16),
        ],
        6 * MIB,
    )(*pieces, *gains)


def on_device(attn_heads, out_weight, residual, norm_gain):
    tensor = lax.axis_size("tensor")
    rows, block = residual.shape
    swap = [(0, 1), (1, 0)]

    def exchange(value, step):
        return lax.ppermute(value, "tensor", [(i, i ^ step) for i in range(tensor)])

    gain = norm_gain.reshape(-1, LANES)
    gain = jnp.pad(gain, ((0, -gain.shape[0] % 16), (0, 0)))
    peer = lax.ppermute(attn_heads, "seq", swap)
    order = list(range(tensor // 2, tensor)) + list(range(1, tensor // 2)) + [0]
    waves = [order[: tensor // 2], order[tensor // 2 :]]
    got = None
    sums = {}
    arrived = {}
    for steps in waves:
        if got is not None:
            peer, _ = lax.optimization_barrier((peer, got))
        keep, give = project(attn_heads, peer, out_weight, tensor, steps)
        got = lax.ppermute(give, "seq", swap)
        sums.update(pair_sum(steps, keep, got, residual, gain))
        for step in steps:
            if step:
                arrived[step] = [exchange(value, step) for value in sums[step]]
    streams = [
        finish_stream(base, [arrived[step][split] for step in range(1, tensor)])
        for split, base in enumerate(sums[0])
    ]
    pieces = list(streams)
    for step in range(1, tensor):
        pieces += [exchange(value, step) for value in streams]
    gains = [gain] + [arrived[step][0] for step in range(1, tensor)]
    stream, normed = normalize(pieces, gains, rows, block)
    return stream, normed


def solution(mesh):
    in_specs = (
        P(("groups", "dp", "seq"), "tensor"),
        P(("tensor", "seq"), None),
        P(("groups", "dp", "seq"), "tensor"),
        P("tensor"),
    )
    out_specs = (P(("groups", "dp", "seq"), "tensor"), P(("groups", "dp", "seq"), None))

    return jax.shard_map(on_device, mesh=mesh, in_specs=in_specs, out_specs=out_specs, check_vma=False)
```

```python
import functools

import jax
import jax.numpy as jnp
from jax import lax
from jax.experimental import pallas as pl
from jax.experimental.pallas import tpu as pltpu
from jax.sharding import PartitionSpec as P


VMEM, HBM = pltpu.VMEM, pltpu.HBM
MIB = 1024 * 1024
F32, BF16 = jnp.float32, jnp.bfloat16
LANES = 128
SPLITS = 1
READY = 2


def call(kernel, in_specs, out_shape, limit, scratch=()):
    return pl.pallas_call(
        kernel,
        in_specs=[pl.BlockSpec(memory_space=space) for space in in_specs],
        out_specs=[pl.BlockSpec(memory_space=VMEM)] * len(out_shape),
        out_shape=out_shape,
        scratch_shapes=list(scratch),
        compiler_params=pltpu.CompilerParams(vmem_limit_bytes=limit),
    )


def chunk_copies(tensor, chunk, steps, weight):
    block = weight.shape[1] // tensor
    rank = lax.axis_index("tensor")
    copies = []
    for step in steps:
        for piece in range(block // chunk):
            start = pl.multiple_of((rank ^ step) * block + piece * chunk, LANES)
            copies.append(functools.partial(pltpu.make_async_copy, weight.at[:, pl.ds(start, chunk)]))
    return copies


def prefetch_kernel(tensor, chunk, steps, own_hbm, weight, own_ref, ready_ref, own_sem, sems):
    depth = weight.shape[0]
    features = pl.ds(pl.multiple_of(lax.axis_index("seq") * depth, LANES), depth)
    own_copy = pltpu.make_async_copy(own_hbm.at[:, features], own_ref, own_sem)
    own_copy.start()
    copies = chunk_copies(tensor, chunk, steps, weight)[: ready_ref.shape[0]]
    copies = [copy(ready_ref.at[i], sems.at[i]) for i, copy in enumerate(copies)]
    for copy in copies:
        copy.start()
    for copy in copies:
        copy.wait()
    own_copy.wait()


def refill_kernel(tensor, chunk, steps, _, weight, ready_ref, sems):
    copies = chunk_copies(tensor, chunk, steps, weight)[: ready_ref.shape[0]]
    copies = [copy(ready_ref.at[i], sems.at[i]) for i, copy in enumerate(copies)]
    for copy in copies:
        copy.start()
    for copy in copies:
        copy.wait()


def project_kernel(tensor, chunk, steps, own_ref, peer_ref, ready_ref, weight, keep_ref, give_ref, held, sems):
    depth, width = weight.shape
    block = width // tensor
    per_block = block // chunk
    early = ready_ref.shape[0]
    copies = chunk_copies(tensor, chunk, steps, weight)[early:]
    copies = [copy(held.at[i], sems.at[i]) for i, copy in enumerate(copies)]
    for copy in copies:
        copy.start()
    features = pl.ds(pl.multiple_of(lax.axis_index("seq") * depth, LANES), depth)
    rows = own_ref.shape[0]
    operand = jnp.concatenate([own_ref[...], peer_ref[:, features]], axis=0)
    for index in range(len(steps) * per_block):
        place, piece = divmod(index, per_block)
        if index < early:
            right = ready_ref[index]
        else:
            copies[index - early].wait()
            right = held[index - early]
        product = jnp.dot(operand, right, preferred_element_type=F32)
        columns = pl.ds(piece * chunk, chunk)
        keep_ref[place, :, columns] = product[:rows]
        give_ref[place, :, columns] = product[rows:].astype(BF16)


def chunk_of(weight, tensor):
    block = weight.shape[1] // tensor
    chunk = min(block, 512)
    return chunk, min(READY * MIB // (2 * weight.shape[0] * chunk), block // chunk)


def prefetch(own, weight, tensor, steps):
    rows, depth = own.shape[0], weight.shape[0]
    chunk, early = chunk_of(weight, tensor)
    return call(
        functools.partial(prefetch_kernel, tensor, chunk, steps),
        [HBM, HBM],
        [
            jax.ShapeDtypeStruct((rows, depth), BF16),
            jax.ShapeDtypeStruct((early, depth, chunk), BF16),
        ],
        2 * depth * chunk * early + 2 * MIB,
        [pltpu.SemaphoreType.DMA(()), pltpu.SemaphoreType.DMA((early,))],
    )(pltpu.with_memory_space_constraint(own, HBM), pltpu.with_memory_space_constraint(weight, HBM))


def refill(after, weight, tensor, steps):
    depth = weight.shape[0]
    chunk, early = chunk_of(weight, tensor)
    return call(
        functools.partial(refill_kernel, tensor, chunk, steps),
        [VMEM, HBM],
        [jax.ShapeDtypeStruct((early, depth, chunk), BF16)],
        2 * depth * chunk * early + 2 * MIB,
        [pltpu.SemaphoreType.DMA((early,))],
    )(after, pltpu.with_memory_space_constraint(weight, HBM))[0]


def project(own, peer, ready, weight, tensor, steps):
    rows = own.shape[0]
    depth, width = weight.shape
    block = width // tensor
    chunk, early = chunk_of(weight, tensor)
    count = len(steps) * block // chunk - early
    return call(
        functools.partial(project_kernel, tensor, chunk, steps),
        [VMEM, VMEM, VMEM, HBM],
        [
            jax.ShapeDtypeStruct((len(steps), rows, block), F32),
            jax.ShapeDtypeStruct((len(steps), rows, block), BF16),
        ],
        2 * depth * chunk * (count + early) + 4 * MIB,
        [VMEM((count, depth, chunk), BF16), pltpu.SemaphoreType.DMA((count,))],
    )(own, peer, ready, pltpu.with_memory_space_constraint(weight, HBM))


def pair_kernel(steps, keep_ref, got_ref, residual_ref, gain_ref, *out_refs):
    _, rows, block = keep_ref.shape
    part = rows // SPLITS
    targets = iter(out_refs)
    for place, step in enumerate(steps):
        for split in range(SPLITS):
            target = next(targets)
            span = slice(split * part, (split + 1) * part)
            for tile in range(block // LANES):
                columns = slice(tile * LANES, (tile + 1) * LANES)
                value = keep_ref[place, span, columns] + got_ref[place, span, columns].astype(F32)
                if step == 0:
                    value = value + residual_ref[span, columns].astype(F32)
                target[tile * part : (tile + 1) * part, :] = value.astype(target.dtype)
            if step and not split:
                target[block // LANES * part :, :] = gain_ref[...]


def pair_sum(steps, keep, got, residual, gain):
    _, rows, block = keep.shape
    length = rows // SPLITS * block // LANES
    shapes = []
    for step in steps:
        for split in range(SPLITS):
            extra = gain.shape[0] if step and not split else 0
            shapes.append(jax.ShapeDtypeStruct((length + extra, LANES), BF16 if step else F32))
    outs = call(functools.partial(pair_kernel, steps), [VMEM] * 4, shapes, 6 * MIB)(keep, got, residual, gain)
    return {step: outs[i * SPLITS : (i + 1) * SPLITS] for i, step in enumerate(steps)}


def stream_kernel(base_ref, *refs):
    length = base_ref.shape[0]
    total = base_ref[...]
    for ref in refs[:-1]:
        total = total + ref[:length, :].astype(F32)
    refs[-1][...] = total.astype(BF16)


def finish_stream(base, parts):
    return call(
        stream_kernel, [VMEM] * (1 + len(parts)), [jax.ShapeDtypeStruct(base.shape, BF16)], 4 * MIB
    )(base, *parts)[0]


def norm_kernel(tensor, rows, block, *refs):
    pieces, refs = refs[: tensor * SPLITS], refs[tensor * SPLITS :]
    gains, (stream_ref, out_ref) = refs[:tensor], refs[tensor:]
    part = rows // SPLITS
    tiles = block // LANES
    rank = lax.axis_index("tensor")
    starts = [(rank ^ step) * block for step in range(tensor)]
    gain_rows = []
    for step, ref in enumerate(gains):
        first = tiles * part if step else 0
        gain_rows.append(ref[first:, :].astype(F32))
    for split in range(SPLITS):
        span = slice(split * part, (split + 1) * part)
        total = jnp.zeros((part, LANES), F32)
        for step in range(tensor):
            for tile in range(tiles):
                value = pieces[step * SPLITS + split][tile * part : (tile + 1) * part, :].astype(F32)
                total = total + value * value
        mean_square = jnp.sum(total, axis=1, keepdims=True) / (tensor * block)
        scale = jnp.broadcast_to(lax.rsqrt(mean_square + 1e-05), (part, LANES))
        for step in range(tensor):
            for tile in range(tiles):
                piece = pieces[step * SPLITS + split][tile * part : (tile + 1) * part, :]
                value = piece.astype(F32) * scale * gain_rows[step][tile : tile + 1, :]
                columns = pl.ds(pl.multiple_of(starts[step] + tile * LANES, LANES), LANES)
                out_ref[span, columns] = value.astype(BF16)
                if step == 0:
                    stream_ref[span, tile * LANES : (tile + 1) * LANES] = piece


def normalize(pieces, gains, rows, block):
    tensor = len(gains)
    return call(
        functools.partial(norm_kernel, tensor, rows, block),
        [VMEM] * (tensor * SPLITS + tensor),
        [
            jax.ShapeDtypeStruct((rows, block), BF16),
            jax.ShapeDtypeStruct((rows, tensor * block), BF16),
        ],
        6 * MIB,
    )(*pieces, *gains)


def on_device(attn_heads, out_weight, residual, norm_gain):
    tensor = lax.axis_size("tensor")
    rows, block = residual.shape
    swap = [(0, 1), (1, 0)]

    def exchange(value, step):
        return lax.ppermute(value, "tensor", [(i, i ^ step) for i in range(tensor)])

    gain = norm_gain.reshape(-1, LANES)
    gain = jnp.pad(gain, ((0, -gain.shape[0] % 16), (0, 0)))
    order = list(range(tensor // 2, tensor)) + list(range(1, tensor // 2)) + [0]
    waves = [order[: tensor // 2], order[tensor // 2 :]]
    peer = lax.ppermute(attn_heads, "seq", swap)
    own, ready = prefetch(attn_heads, out_weight, tensor, waves[0])
    sums = {}
    arrived = {}
    for wave, steps in enumerate(waves):
        keep, give = project(own, peer, ready, out_weight, tensor, steps)
        got = lax.ppermute(give, "seq", swap)
        if wave == 0:
            own, _ = lax.optimization_barrier((own, give))
            ready = refill(own, out_weight, tensor, waves[1])
            peer, _ = lax.optimization_barrier((peer, got))
        sums.update(pair_sum(steps, keep, got, residual, gain))
        for step in steps:
            if step:
                arrived[step] = [exchange(value, step) for value in sums[step]]
    streams = [
        finish_stream(base, [arrived[step][split] for step in range(1, tensor)])
        for split, base in enumerate(sums[0])
    ]
    pieces = list(streams)
    for step in range(1, tensor):
        pieces += [exchange(value, step) for value in streams]
    gains = [gain] + [arrived[step][0] for step in range(1, tensor)]
    stream, normed = normalize(pieces, gains, rows, block)
    return stream, normed


def solution(mesh):
    in_specs = (
        P(("groups", "dp", "seq"), "tensor"),
        P(("tensor", "seq"), None),
        P(("groups", "dp", "seq"), "tensor"),
        P("tensor"),
    )
    out_specs = (P(("groups", "dp", "seq"), "tensor"), P(("groups", "dp", "seq"), None))

    return jax.shard_map(on_device, mesh=mesh, in_specs=in_specs, out_specs=out_specs, check_vma=False)
```

```python
import functools

import jax
import jax.numpy as jnp
from jax import lax
from jax.experimental import pallas as pl
from jax.experimental.pallas import tpu as pltpu
from jax.sharding import PartitionSpec as P


VMEM, HBM = pltpu.VMEM, pltpu.HBM
MIB = 1024 * 1024
F32, BF16 = jnp.float32, jnp.bfloat16
LANES = 128
READY = 2
CHUNK = 512


def call(kernel, in_specs, out_shape, limit, scratch=()):
    return pl.pallas_call(
        kernel,
        in_specs=[pl.BlockSpec(memory_space=space) for space in in_specs],
        out_specs=[pl.BlockSpec(memory_space=VMEM)] * len(out_shape),
        out_shape=out_shape,
        scratch_shapes=list(scratch),
        compiler_params=pltpu.CompilerParams(vmem_limit_bytes=limit),
    )


def chunk_copies(tensor, chunk, steps, weight):
    block = weight.shape[1] // tensor
    rank = lax.axis_index("tensor")
    copies = []
    for step in steps:
        for piece in range(block // chunk):
            start = pl.multiple_of((rank ^ step) * block + piece * chunk, LANES)
            copies.append(functools.partial(pltpu.make_async_copy, weight.at[:, pl.ds(start, chunk)]))
    return copies


def prefetch_kernel(tensor, chunk, steps, own_hbm, weight, own_ref, ready_ref, own_sem, sems):
    depth = weight.shape[0]
    features = pl.ds(pl.multiple_of(lax.axis_index("seq") * depth, LANES), depth)
    own_copy = pltpu.make_async_copy(own_hbm.at[:, features], own_ref, own_sem)
    own_copy.start()
    copies = chunk_copies(tensor, chunk, steps, weight)[: ready_ref.shape[0]]
    copies = [copy(ready_ref.at[i], sems.at[i]) for i, copy in enumerate(copies)]
    for copy in copies:
        copy.start()
    for copy in copies:
        copy.wait()
    own_copy.wait()


def refill_kernel(tensor, chunk, steps, _, weight, ready_ref, sems):
    copies = chunk_copies(tensor, chunk, steps, weight)[: ready_ref.shape[0]]
    copies = [copy(ready_ref.at[i], sems.at[i]) for i, copy in enumerate(copies)]
    for copy in copies:
        copy.start()
    for copy in copies:
        copy.wait()


def project_kernel(tensor, chunk, steps, own_ref, peer_ref, ready_ref, weight, keep_ref, give_ref, held, sems):
    depth, width = weight.shape
    block = width // tensor
    per_block = block // chunk
    early = ready_ref.shape[0]
    copies = chunk_copies(tensor, chunk, steps, weight)[early:]
    copies = [copy(held.at[i], sems.at[i]) for i, copy in enumerate(copies)]
    for copy in copies:
        copy.start()
    features = pl.ds(pl.multiple_of(lax.axis_index("seq") * depth, LANES), depth)
    rows = own_ref.shape[0]
    operand = jnp.concatenate([own_ref[...], peer_ref[:, features]], axis=0)
    for index in range(len(steps) * per_block):
        place, piece = divmod(index, per_block)
        if index < early:
            right = ready_ref[index]
        else:
            copies[index - early].wait()
            right = held[index - early]
        product = jnp.dot(operand, right, preferred_element_type=F32)
        columns = pl.ds(piece * chunk, chunk)
        keep_ref[place, :, columns] = product[:rows]
        give_ref[place, :, columns] = product[rows:].astype(BF16)


def chunk_of(weight, tensor):
    block = weight.shape[1] // tensor
    chunk = min(block, CHUNK)
    return chunk, min(READY * MIB // (2 * weight.shape[0] * chunk), block // chunk)


def prefetch(own, weight, tensor, steps):
    rows, depth = own.shape[0], weight.shape[0]
    chunk, early = chunk_of(weight, tensor)
    return call(
        functools.partial(prefetch_kernel, tensor, chunk, steps),
        [HBM, HBM],
        [
            jax.ShapeDtypeStruct((rows, depth), BF16),
            jax.ShapeDtypeStruct((early, depth, chunk), BF16),
        ],
        2 * depth * chunk * early + 2 * MIB,
        [pltpu.SemaphoreType.DMA(()), pltpu.SemaphoreType.DMA((early,))],
    )(pltpu.with_memory_space_constraint(own, HBM), pltpu.with_memory_space_constraint(weight, HBM))


def refill(after, weight, tensor, steps):
    depth = weight.shape[0]
    chunk, early = chunk_of(weight, tensor)
    return call(
        functools.partial(refill_kernel, tensor, chunk, steps),
        [VMEM, HBM],
        [jax.ShapeDtypeStruct((early, depth, chunk), BF16)],
        2 * depth * chunk * early + 2 * MIB,
        [pltpu.SemaphoreType.DMA((early,))],
    )(after, pltpu.with_memory_space_constraint(weight, HBM))[0]


def project(own, peer, ready, weight, tensor, steps):
    rows = own.shape[0]
    depth, width = weight.shape
    block = width // tensor
    chunk, early = chunk_of(weight, tensor)
    count = len(steps) * block // chunk - early
    return call(
        functools.partial(project_kernel, tensor, chunk, steps),
        [VMEM, VMEM, VMEM, HBM],
        [
            jax.ShapeDtypeStruct((len(steps), rows, block), F32),
            jax.ShapeDtypeStruct((len(steps), rows, block), BF16),
        ],
        2 * depth * chunk * (count + early) + 4 * MIB,
        [VMEM((count, depth, chunk), BF16), pltpu.SemaphoreType.DMA((count,))],
    )(own, peer, ready, pltpu.with_memory_space_constraint(weight, HBM))


def pair_kernel(steps, keep_ref, got_ref, residual_ref, gain_ref, *out_refs):
    _, rows, block = keep_ref.shape
    for place, step in enumerate(steps):
        target = out_refs[place]
        for tile in range(block // LANES):
            columns = slice(tile * LANES, (tile + 1) * LANES)
            value = keep_ref[place, :, columns] + got_ref[place, :, columns].astype(F32)
            if step == 0:
                value = value + residual_ref[:, columns].astype(F32)
            target[tile * rows : (tile + 1) * rows, :] = value.astype(target.dtype)
        if step:
            target[block // LANES * rows :, :] = gain_ref[...]


def pair_sum(steps, keep, got, residual, gain):
    _, rows, block = keep.shape
    length = rows * block // LANES
    shapes = [
        jax.ShapeDtypeStruct((length + gain.shape[0], LANES), BF16)
        if step
        else jax.ShapeDtypeStruct((length, LANES), F32)
        for step in steps
    ]
    outs = call(functools.partial(pair_kernel, steps), [VMEM] * 4, shapes, 6 * MIB)(
        keep, got, residual, gain
    )
    return dict(zip(steps, outs))


def stream_kernel(count, base_ref, *refs):
    length = base_ref.shape[0]
    total = base_ref[...]
    for ref in refs[:count]:
        total = total + ref[:length, :].astype(F32)
    stream = total.astype(BF16)
    refs[count][...] = stream
    for half, ref in enumerate(refs[count + 1 :]):
        ref[...] = stream[half * length // 2 : (half + 1) * length // 2]


def finish_stream(base, parts, halves):
    length = base.shape[0]
    shapes = [jax.ShapeDtypeStruct(base.shape, BF16)]
    if halves:
        shapes += [jax.ShapeDtypeStruct((length // 2, LANES), BF16)] * 2
    return call(
        functools.partial(stream_kernel, len(parts)), [VMEM] * (1 + len(parts)), shapes, 4 * MIB
    )(base, *parts)


def norm_kernel(rows, block, counts, *refs):
    tensor = len(counts)
    tiles = block // LANES
    refs = list(refs)
    pieces = []
    for count in counts:
        group = [refs.pop(0) for _ in range(count)]
        size = tiles // count
        pieces.append([(group[tile // size], tile % size) for tile in range(tiles)])
    gains, (stream_ref, out_ref) = refs[:tensor], refs[tensor:]
    rank = lax.axis_index("tensor")
    total = jnp.zeros((rows, LANES), F32)
    for piece in pieces:
        for ref, tile in piece:
            value = ref[tile * rows : (tile + 1) * rows, :].astype(F32)
            total = total + value * value
    mean_square = jnp.sum(total, axis=1, keepdims=True) / (tensor * block)
    scale = jnp.broadcast_to(lax.rsqrt(mean_square + 1e-05), (rows, LANES))
    for step, piece in enumerate(pieces):
        gain = gains[step][tiles * rows if step else 0 :, :].astype(F32)
        for index, (ref, tile) in enumerate(piece):
            value = ref[tile * rows : (tile + 1) * rows, :]
            start = pl.multiple_of((rank ^ step) * block + index * LANES, LANES)
            scaled = value.astype(F32) * scale * gain[index : index + 1, :]
            out_ref[:, pl.ds(start, LANES)] = scaled.astype(BF16)
            if step == 0:
                stream_ref[:, index * LANES : (index + 1) * LANES] = value


def normalize(pieces, gains, rows, block):
    tensor = len(gains)
    flat = [part for piece in pieces for part in piece]
    return call(
        functools.partial(norm_kernel, rows, block, [len(piece) for piece in pieces]),
        [VMEM] * (len(flat) + tensor),
        [
            jax.ShapeDtypeStruct((rows, block), BF16),
            jax.ShapeDtypeStruct((rows, tensor * block), BF16),
        ],
        6 * MIB,
    )(*flat, *gains)


def on_device(attn_heads, out_weight, residual, norm_gain):
    tensor = lax.axis_size("tensor")
    rows, block = residual.shape
    swap = [(0, 1), (1, 0)]

    def exchange(value, step):
        return lax.ppermute(value, "tensor", [(i, i ^ step) for i in range(tensor)])

    gain = norm_gain.reshape(-1, LANES)
    gain = jnp.pad(gain, ((0, -gain.shape[0] % 16), (0, 0)))
    order = list(range(tensor // 2, tensor)) + list(range(1, tensor // 2)) + [0]
    waves = [order[: tensor // 2], order[tensor // 2 :]]
    peer = lax.ppermute(attn_heads, "seq", swap)
    own, ready = prefetch(attn_heads, out_weight, tensor, waves[0])
    sums = {}
    arrived = {}
    for wave, steps in enumerate(waves):
        keep, give = project(own, peer, ready, out_weight, tensor, steps)
        got = lax.ppermute(give, "seq", swap)
        if wave == 0:
            own, _ = lax.optimization_barrier((own, give))
            ready = refill(own, out_weight, tensor, waves[1])
            peer, _ = lax.optimization_barrier((peer, got))
        sums.update(pair_sum(steps, keep, got, residual, gain))
        for step in steps:
            if step:
                arrived[step] = exchange(sums[step], step)
    parts = [arrived[step] for step in range(1, tensor)]
    stream, *halves = finish_stream(sums[0], parts, tensor == 4)
    pieces = [[stream]] + [None] * (tensor - 1)
    if halves:
        first, second = halves
        relayed = exchange(first, 2)
        pieces[1] = [exchange(stream, 1)]
        pieces[2] = [relayed, exchange(second, 2)]
        direct = exchange(second, 3)
        pieces[3] = [exchange(relayed, 1), direct]
    else:
        for step in range(1, tensor):
            pieces[step] = [exchange(stream, step)]
    return normalize(pieces, [gain] + parts, rows, block)


def solution(mesh):
    in_specs = (
        P(("groups", "dp", "seq"), "tensor"),
        P(("tensor", "seq"), None),
        P(("groups", "dp", "seq"), "tensor"),
        P("tensor"),
    )
    out_specs = (P(("groups", "dp", "seq"), "tensor"), P(("groups", "dp", "seq"), None))

    return jax.shard_map(on_device, mesh=mesh, in_specs=in_specs, out_specs=out_specs, check_vma=False)
```

```python
import functools

import jax
import jax.numpy as jnp
from jax import lax
from jax.experimental import pallas as pl
from jax.experimental.pallas import tpu as pltpu
from jax.sharding import PartitionSpec as P


VMEM, HBM = pltpu.VMEM, pltpu.HBM
MIB = 1024 * 1024
F32, BF16 = jnp.float32, jnp.bfloat16
LANES = 128
READY = 2
CHUNK = 512


def call(kernel, in_specs, out_shape, limit, scratch=()):
    return pl.pallas_call(
        kernel,
        in_specs=[pl.BlockSpec(memory_space=space) for space in in_specs],
        out_specs=[pl.BlockSpec(memory_space=VMEM)] * len(out_shape),
        out_shape=out_shape,
        scratch_shapes=list(scratch),
        compiler_params=pltpu.CompilerParams(vmem_limit_bytes=limit),
    )


def chunk_copies(tensor, chunk, steps, weight):
    block = weight.shape[1] // tensor
    rank = lax.axis_index("tensor")
    copies = []
    for step in steps:
        for piece in range(block // chunk):
            start = pl.multiple_of((rank ^ step) * block + piece * chunk, LANES)
            copies.append(functools.partial(pltpu.make_async_copy, weight.at[:, pl.ds(start, chunk)]))
    return copies


def prefetch_kernel(tensor, chunk, steps, own_hbm, weight, own_ref, ready_ref, own_sem, sems):
    depth = weight.shape[0]
    features = pl.ds(pl.multiple_of(lax.axis_index("seq") * depth, LANES), depth)
    own_copy = pltpu.make_async_copy(own_hbm.at[:, features], own_ref, own_sem)
    own_copy.start()
    copies = chunk_copies(tensor, chunk, steps, weight)[: ready_ref.shape[0]]
    copies = [copy(ready_ref.at[i], sems.at[i]) for i, copy in enumerate(copies)]
    for copy in copies:
        copy.start()
    for copy in copies:
        copy.wait()
    own_copy.wait()


def refill_kernel(tensor, chunk, steps, _, weight, ready_ref, sems):
    copies = chunk_copies(tensor, chunk, steps, weight)[: ready_ref.shape[0]]
    copies = [copy(ready_ref.at[i], sems.at[i]) for i, copy in enumerate(copies)]
    for copy in copies:
        copy.start()
    for copy in copies:
        copy.wait()


def project_kernel(tensor, chunk, steps, early, own_ref, peer_ref, *refs):
    *ready_refs, weight, keep_ref, give_ref, held, sems = refs
    depth, width = weight.shape
    block = width // tensor
    per_block = block // chunk
    copies = chunk_copies(tensor, chunk, steps, weight)[early:]
    copies = [copy(held.at[i], sems.at[i]) for i, copy in enumerate(copies)]
    for copy in copies:
        copy.start()
    features = pl.ds(pl.multiple_of(lax.axis_index("seq") * depth, LANES), depth)
    rows = own_ref.shape[0]
    operand = jnp.concatenate([own_ref[...], peer_ref[:, features]], axis=0)
    for index in range(len(steps) * per_block):
        place, piece = divmod(index, per_block)
        if index < early:
            right = ready_refs[0][index]
        else:
            copies[index - early].wait()
            right = held[index - early]
        product = jnp.dot(operand, right, preferred_element_type=F32)
        columns = pl.ds(piece * chunk, chunk)
        keep_ref[place, :, columns] = product[:rows]
        give_ref[place, :, columns] = product[rows:].astype(BF16)


def chunk_of(weight, tensor):
    block = weight.shape[1] // tensor
    chunk = min(block, CHUNK)
    return chunk, min(READY * MIB // (2 * weight.shape[0] * chunk), block // chunk)


def prefetch(own, weight, tensor, steps):
    rows, depth = own.shape[0], weight.shape[0]
    chunk, early = chunk_of(weight, tensor)
    return call(
        functools.partial(prefetch_kernel, tensor, chunk, steps),
        [HBM, HBM],
        [
            jax.ShapeDtypeStruct((rows, depth), BF16),
            jax.ShapeDtypeStruct((early, depth, chunk), BF16),
        ],
        2 * depth * chunk * early + 2 * MIB,
        [pltpu.SemaphoreType.DMA(()), pltpu.SemaphoreType.DMA((early,))],
    )(pltpu.with_memory_space_constraint(own, HBM), pltpu.with_memory_space_constraint(weight, HBM))


def refill(after, weight, tensor, steps):
    depth = weight.shape[0]
    chunk, early = chunk_of(weight, tensor)
    return call(
        functools.partial(refill_kernel, tensor, chunk, steps),
        [VMEM, HBM],
        [jax.ShapeDtypeStruct((early, depth, chunk), BF16)],
        2 * depth * chunk * early + 2 * MIB,
        [pltpu.SemaphoreType.DMA((early,))],
    )(after, pltpu.with_memory_space_constraint(weight, HBM))[0]


def project(own, peer, ready, weight, tensor, steps):
    rows = own.shape[0]
    depth, width = weight.shape
    block = width // tensor
    chunk, early = chunk_of(weight, tensor)
    ready = [] if ready is None else [ready]
    early = early if ready else 0
    count = len(steps) * block // chunk - early
    return call(
        functools.partial(project_kernel, tensor, chunk, steps, early),
        [VMEM] * (2 + len(ready)) + [HBM],
        [
            jax.ShapeDtypeStruct((len(steps), rows, block), F32),
            jax.ShapeDtypeStruct((len(steps), rows, block), BF16),
        ],
        2 * depth * chunk * (count + early) + 4 * MIB,
        [VMEM((count, depth, chunk), BF16), pltpu.SemaphoreType.DMA((count,))],
    )(own, peer, *ready, pltpu.with_memory_space_constraint(weight, HBM))


def pair_kernel(plan, keep_ref, got_ref, gain_ref, *out_refs):
    rows = keep_ref.shape[1]
    for (place, first, last, gained), target in zip(plan, out_refs):
        for tile in range(first, last):
            columns = slice(tile * LANES, (tile + 1) * LANES)
            value = keep_ref[place, :, columns] + got_ref[place, :, columns].astype(F32)
            target[(tile - first) * rows : (tile - first + 1) * rows, :] = value.astype(target.dtype)
        if gained:
            target[(last - first) * rows :, :] = gain_ref[...]


def pair_sum(plan, keep, got, gain):
    rows = keep.shape[1]
    shapes = [
        jax.ShapeDtypeStruct(((last - first) * rows + gained * gain.shape[0], LANES), dtype)
        for _, first, last, gained, dtype in plan
    ]
    kernel = functools.partial(pair_kernel, [entry[:4] for entry in plan])
    return call(kernel, [VMEM] * 3, shapes, 6 * MIB)(keep, got, gain)


def relay_kernel(mine_ref, got_ref, out_ref):
    out_ref[...] = (mine_ref[...] + got_ref[...].astype(F32)).astype(BF16)


def relay_sum(mine, got):
    shapes = [jax.ShapeDtypeStruct(mine.shape, BF16)]
    return call(relay_kernel, [VMEM] * 2, shapes, 4 * MIB)(mine, got)[0]


def stream_kernel(spans, keep_ref, got_ref, residual_ref, *refs):
    _, rows, block = keep_ref.shape
    parts, stream_ref, halves = refs[: len(spans)], refs[len(spans)], refs[len(spans) + 1 :]
    tiles = block // LANES
    for tile in range(tiles):
        columns = slice(tile * LANES, (tile + 1) * LANES)
        value = keep_ref[0, :, columns] + got_ref[0, :, columns].astype(F32)
        value = value + residual_ref[:, columns].astype(F32)
        for (first, last), part in zip(spans, parts):
            if first <= tile < last:
                value = value + part[(tile - first) * rows : (tile - first + 1) * rows, :].astype(F32)
        stream = value.astype(BF16)
        stream_ref[tile * rows : (tile + 1) * rows, :] = stream
        if halves:
            half, index = divmod(tile, tiles // 2)
            halves[half][index * rows : (index + 1) * rows, :] = stream


def finish_stream(keep, got, residual, parts, spans, halves):
    _, rows, block = keep.shape
    length = rows * block // LANES
    shapes = [jax.ShapeDtypeStruct((length, LANES), BF16)]
    if halves:
        shapes += [jax.ShapeDtypeStruct((length // 2, LANES), BF16)] * 2
    return call(
        functools.partial(stream_kernel, spans), [VMEM] * (3 + len(parts)), shapes, 4 * MIB
    )(keep, got, residual, *parts)


def norm_kernel(rows, block, counts, gain_rows, *refs):
    tensor = len(counts)
    tiles = block // LANES
    refs = list(refs)
    pieces = []
    for count in counts:
        group = [refs.pop(0) for _ in range(count)]
        size = tiles // count
        pieces.append([(group[tile // size], tile % size) for tile in range(tiles)])
    gains, (stream_ref, out_ref) = refs[:tensor], refs[tensor:]
    rank = lax.axis_index("tensor")
    total = jnp.zeros((rows, LANES), F32)
    for piece in pieces:
        for ref, tile in piece:
            value = ref[tile * rows : (tile + 1) * rows, :].astype(F32)
            total = total + value * value
    mean_square = jnp.sum(total, axis=1, keepdims=True) / (tensor * block)
    scale = jnp.broadcast_to(lax.rsqrt(mean_square + 1e-05), (rows, LANES))
    for step, piece in enumerate(pieces):
        gain = gains[step][gains[step].shape[0] - gain_rows :, :].astype(F32)
        for index, (ref, tile) in enumerate(piece):
            value = ref[tile * rows : (tile + 1) * rows, :]
            start = pl.multiple_of((rank ^ step) * block + index * LANES, LANES)
            scaled = value.astype(F32) * scale * gain[index : index + 1, :]
            out_ref[:, pl.ds(start, LANES)] = scaled.astype(BF16)
            if step == 0:
                stream_ref[:, index * LANES : (index + 1) * LANES] = value


def normalize(pieces, gains, rows, block):
    tensor = len(gains)
    flat = [part for piece in pieces for part in piece]
    return call(
        functools.partial(
            norm_kernel, rows, block, [len(piece) for piece in pieces], gains[0].shape[0]
        ),
        [VMEM] * (len(flat) + tensor),
        [
            jax.ShapeDtypeStruct((rows, block), BF16),
            jax.ShapeDtypeStruct((rows, tensor * block), BF16),
        ],
        6 * MIB,
    )(*flat, *gains)


def on_device(attn_heads, out_weight, residual, norm_gain):
    tensor = lax.axis_size("tensor")
    rows, block = residual.shape
    swap = [(0, 1), (1, 0)]

    def exchange(value, step):
        return lax.ppermute(value, "tensor", [(i, i ^ step) for i in range(tensor)])

    gain = norm_gain.reshape(-1, LANES)
    gain = jnp.pad(gain, ((0, -gain.shape[0] % 16), (0, 0)))
    relay = tensor == 4
    waves = [list(range(tensor - 1, 0, -1)), [0]]
    tiles = block // LANES
    half = tiles // 2
    peer = lax.ppermute(attn_heads, "seq", swap)
    own, ready = prefetch(attn_heads, out_weight, tensor, waves[0])
    parts = []
    spans = []
    gains = [gain] + [None] * (tensor - 1)

    def receive(part, first, last):
        parts.append(part)
        spans.append((first, last))
        return part

    for wave, steps in enumerate(waves):
        keep, give = project(own, peer, ready, out_weight, tensor, steps)
        got = lax.ppermute(give, "seq", swap)
        if wave:
            break
        own, _ = lax.optimization_barrier((own, give))
        ready = refill(own, out_weight, tensor, waves[1])
        peer, _ = lax.optimization_barrier((peer, got))
        if relay:
            plan = [
                (0, 0, half, False, BF16),
                (1, half, tiles, True, BF16),
                (0, half, tiles, True, BF16),
                (2, 0, tiles, True, BF16),
                (1, 0, half, False, F32),
            ]
            away, near, far, beside, mine = pair_sum(plan, keep, got, gain)
            relayed = exchange(away, 1)
            gains[2] = receive(exchange(near, 2), half, tiles)
            gains[3] = receive(exchange(far, 3), half, tiles)
            gains[1] = receive(exchange(beside, 1), 0, tiles)
            through = relay_sum(mine, relayed)
            receive(exchange(through, 2), 0, half)
        else:
            plan = [(place, 0, tiles, True, BF16) for place in range(len(steps))]
            for step, value in zip(steps, pair_sum(plan, keep, got, gain)):
                gains[step] = receive(exchange(value, step), 0, tiles)
    stream, *halves = finish_stream(keep, got, residual, parts, spans, relay)
    pieces = [[stream]] + [None] * (tensor - 1)
    if halves:
        first, second = halves
        relayed = exchange(first, 2)
        pieces[1] = [exchange(stream, 1)]
        pieces[2] = [relayed, exchange(second, 2)]
        direct = exchange(second, 3)
        pieces[3] = [exchange(relayed, 1), direct]
    else:
        for step in range(1, tensor):
            pieces[step] = [exchange(stream, step)]
    return normalize(pieces, gains, rows, block)


def solution(mesh):
    in_specs = (
        P(("groups", "dp", "seq"), "tensor"),
        P(("tensor", "seq"), None),
        P(("groups", "dp", "seq"), "tensor"),
        P("tensor"),
    )
    out_specs = (P(("groups", "dp", "seq"), "tensor"), P(("groups", "dp", "seq"), None))

    return jax.shard_map(on_device, mesh=mesh, in_specs=in_specs, out_specs=out_specs, check_vma=False)
```

```python
import functools

import jax
import jax.numpy as jnp
from jax import lax
from jax.experimental import pallas as pl
from jax.experimental.pallas import tpu as pltpu
from jax.sharding import PartitionSpec as P


VMEM, HBM = pltpu.VMEM, pltpu.HBM
MIB = 1024 * 1024
F32, BF16 = jnp.float32, jnp.bfloat16
LANES = 128
READY = 2
LATER = 4
CHUNK = 512


def call(kernel, in_specs, out_shape, limit, scratch=(), out_space=VMEM):
    return pl.pallas_call(
        kernel,
        in_specs=[pl.BlockSpec(memory_space=space) for space in in_specs],
        out_specs=[pl.BlockSpec(memory_space=out_space)] * len(out_shape),
        out_shape=out_shape,
        scratch_shapes=list(scratch),
        compiler_params=pltpu.CompilerParams(vmem_limit_bytes=limit),
    )


def chunk_copies(tensor, chunk, steps, weight):
    block = weight.shape[1] // tensor
    rank = lax.axis_index("tensor")
    copies = []
    for step in steps:
        for piece in range(block // chunk):
            start = pl.multiple_of((rank ^ step) * block + piece * chunk, LANES)
            copies.append(functools.partial(pltpu.make_async_copy, weight.at[:, pl.ds(start, chunk)]))
    return copies


def prefetch_kernel(tensor, chunk, steps, own_hbm, weight, own_ref, ready_ref, own_sem, sems):
    depth = weight.shape[0]
    features = pl.ds(pl.multiple_of(lax.axis_index("seq") * depth, LANES), depth)
    own_copy = pltpu.make_async_copy(own_hbm.at[:, features], own_ref, own_sem)
    own_copy.start()
    copies = chunk_copies(tensor, chunk, steps, weight)[: ready_ref.shape[0]]
    copies = [copy(ready_ref.at[i], sems.at[i]) for i, copy in enumerate(copies)]
    for copy in copies:
        copy.start()
    for copy in copies:
        copy.wait()
    own_copy.wait()


def project_kernel(tensor, chunk, steps, early, after, own_ref, peer_ref, *refs):
    ready_refs, (weight, keep_ref, give_ref, *later_refs, held, sems) = refs[:early], refs[early:]
    depth, width = weight.shape
    block = width // tensor
    per_block = block // chunk
    early = ready_refs[0].shape[0] if early else 0
    copies = chunk_copies(tensor, chunk, steps, weight)[early:]
    copies = [copy(held.at[i], sems.at[i]) for i, copy in enumerate(copies)]
    later = []
    if later_refs:
        later = chunk_copies(tensor, chunk, after, weight)[: later_refs[0].shape[0]]
        later = [copy(later_refs[0].at[i], sems.at[len(copies) + i]) for i, copy in enumerate(later)]
    for copy in copies + later:
        copy.start()
    features = pl.ds(pl.multiple_of(lax.axis_index("seq") * depth, LANES), depth)
    rows = own_ref.shape[0]
    operand = jnp.concatenate([own_ref[...], peer_ref[:, features]], axis=0)
    for index in range(len(steps) * per_block):
        place, piece = divmod(index, per_block)
        if index < early:
            right = ready_refs[0][index]
        else:
            copies[index - early].wait()
            right = held[index - early]
        product = jnp.dot(operand, right, preferred_element_type=F32)
        columns = pl.ds(piece * chunk, chunk)
        keep_ref[place, :, columns] = product[:rows]
        give_ref[place, :, columns] = product[rows:].astype(BF16)
    for copy in later:
        copy.wait()


def chunk_of(weight, tensor):
    block = weight.shape[1] // tensor
    chunk = min(block, CHUNK)
    return chunk, min(READY * MIB // (2 * weight.shape[0] * chunk), block // chunk)


def prefetch(own, weight, tensor, steps):
    rows, depth = own.shape[0], weight.shape[0]
    chunk, early = chunk_of(weight, tensor)
    return call(
        functools.partial(prefetch_kernel, tensor, chunk, steps),
        [HBM, HBM],
        [
            jax.ShapeDtypeStruct((rows, depth), BF16),
            jax.ShapeDtypeStruct((early, depth, chunk), BF16),
        ],
        2 * depth * chunk * early + 2 * MIB,
        [pltpu.SemaphoreType.DMA(()), pltpu.SemaphoreType.DMA((early,))],
    )(pltpu.with_memory_space_constraint(own, HBM), pltpu.with_memory_space_constraint(weight, HBM))


def project(own, peer, ready, weight, tensor, steps, after=()):
    rows = own.shape[0]
    depth, width = weight.shape
    block = width // tensor
    chunk, _ = chunk_of(weight, tensor)
    ready = [] if ready is None else [ready]
    early = ready[0].shape[0] if ready else 0
    count = len(steps) * block // chunk - early
    later = min(LATER * MIB // (2 * depth * chunk), len(after) * block // chunk)
    shapes = [
        jax.ShapeDtypeStruct((len(steps), rows, block), F32),
        jax.ShapeDtypeStruct((len(steps), rows, block), BF16),
    ]
    if later:
        shapes.append(jax.ShapeDtypeStruct((later, depth, chunk), BF16))
    return call(
        functools.partial(project_kernel, tensor, chunk, steps, len(ready), after),
        [VMEM] * (2 + len(ready)) + [HBM],
        shapes,
        2 * depth * chunk * (len(steps) * block // chunk + later) + 4 * MIB,
        [VMEM((count, depth, chunk), BF16), pltpu.SemaphoreType.DMA((count + later,))],
    )(own, peer, *ready, pltpu.with_memory_space_constraint(weight, HBM))


def pair_kernel(plan, keep_ref, got_ref, gain_ref, *out_refs):
    rows = keep_ref.shape[1]
    for (place, first, last, gained), target in zip(plan, out_refs):
        for tile in range(first, last):
            columns = slice(tile * LANES, (tile + 1) * LANES)
            value = keep_ref[place, :, columns] + got_ref[place, :, columns].astype(F32)
            target[(tile - first) * rows : (tile - first + 1) * rows, :] = value.astype(target.dtype)
        if gained:
            target[(last - first) * rows :, :] = gain_ref[...]


def pair_sum(plan, keep, got, gain):
    rows = keep.shape[1]
    shapes = [
        jax.ShapeDtypeStruct(((last - first) * rows + gained * gain.shape[0], LANES), dtype)
        for _, first, last, gained, dtype in plan
    ]
    kernel = functools.partial(pair_kernel, [entry[:4] for entry in plan])
    return call(kernel, [VMEM] * 3, shapes, 6 * MIB)(keep, got, gain)


def relay_kernel(mine_ref, got_ref, out_ref):
    out_ref[...] = (mine_ref[...] + got_ref[...].astype(F32)).astype(BF16)


def relay_sum(mine, got):
    shapes = [jax.ShapeDtypeStruct(mine.shape, BF16)]
    return call(relay_kernel, [VMEM] * 2, shapes, 4 * MIB)(mine, got)[0]


def stream_kernel(spans, first_tile, last_tile, early, keep_ref, got_ref, residual_ref, *refs):
    rows = keep_ref.shape[1]
    parts, refs = refs[: len(spans)], refs[len(spans) :]
    early_refs, (part_ref, *whole_refs) = refs[:early], refs[early:]
    for tile in range(first_tile, last_tile):
        columns = slice(tile * LANES, (tile + 1) * LANES)
        value = keep_ref[0, :, columns] + got_ref[0, :, columns].astype(F32)
        value = value + residual_ref[:, columns].astype(F32)
        for (first, last), part in zip(spans, parts):
            if first <= tile < last:
                value = value + part[(tile - first) * rows : (tile - first + 1) * rows, :].astype(F32)
        stream = value.astype(BF16)
        part_ref[(tile - first_tile) * rows : (tile - first_tile + 1) * rows, :] = stream
        for ref in whole_refs:
            ref[tile * rows : (tile + 1) * rows, :] = stream
    for early_ref, ref in zip(early_refs, whole_refs):
        ref[last_tile * rows :, :] = early_ref[...]


def finish_stream(keep, got, residual, parts, spans, first_tile, last_tile, early=()):
    _, rows, block = keep.shape
    shapes = [jax.ShapeDtypeStruct(((last_tile - first_tile) * rows, LANES), BF16)]
    shapes += [jax.ShapeDtypeStruct((rows * block // LANES, LANES), BF16)] * len(early)
    return call(
        functools.partial(stream_kernel, spans, first_tile, last_tile, len(early)),
        [VMEM] * (3 + len(parts) + len(early)),
        shapes,
        4 * MIB,
    )(keep, got, residual, *parts, *early)


def norm_kernel(rows, block, counts, gain_rows, *refs):
    tensor = len(counts)
    tiles = block // LANES
    refs = list(refs)
    pieces = []
    for count in counts:
        group = [refs.pop(0) for _ in range(count)]
        size = tiles // count
        pieces.append([(group[tile // size], tile % size) for tile in range(tiles)])
    gains, (stream_hbm, out_hbm, stream_ref, out_ref, sems) = refs[:tensor], refs[tensor:]
    rank = lax.axis_index("tensor")
    copies = [pltpu.make_async_copy(stream_ref, stream_hbm, sems.at[tensor])]
    for step in range(tensor):
        start = pl.multiple_of((rank ^ step) * block, LANES)
        target = out_hbm.at[:, pl.ds(start, block)]
        copies.append(pltpu.make_async_copy(out_ref.at[step], target, sems.at[step]))
    for index, (ref, tile) in enumerate(pieces[0]):
        columns = slice(index * LANES, (index + 1) * LANES)
        stream_ref[:, columns] = ref[tile * rows : (tile + 1) * rows, :]
    copies[0].start()
    total = jnp.zeros((rows, LANES), F32)
    for piece in pieces:
        for ref, tile in piece:
            value = ref[tile * rows : (tile + 1) * rows, :].astype(F32)
            total = total + value * value
    mean_square = jnp.sum(total, axis=1, keepdims=True) / (tensor * block)
    scale = jnp.broadcast_to(lax.rsqrt(mean_square + 1e-05), (rows, LANES))
    for step, piece in enumerate(pieces):
        gain = gains[step][gains[step].shape[0] - gain_rows :, :].astype(F32)
        for index, (ref, tile) in enumerate(piece):
            value = ref[tile * rows : (tile + 1) * rows, :].astype(F32)
            scaled = value * scale * gain[index : index + 1, :]
            out_ref[step, :, index * LANES : (index + 1) * LANES] = scaled.astype(BF16)
        copies[step + 1].start()
    for copy in copies:
        copy.wait()


def normalize(pieces, gains, rows, block):
    tensor = len(gains)
    flat = [part for piece in pieces for part in piece]
    counts = [len(piece) for piece in pieces]
    return call(
        functools.partial(norm_kernel, rows, block, counts, gains[0].shape[0]),
        [VMEM] * (len(flat) + tensor),
        [
            jax.ShapeDtypeStruct((rows, block), BF16),
            jax.ShapeDtypeStruct((rows, tensor * block), BF16),
        ],
        6 * MIB,
        [
            VMEM((rows, block), BF16),
            VMEM((tensor, rows, block), BF16),
            pltpu.SemaphoreType.DMA((tensor + 1,)),
        ],
        HBM,
    )(*flat, *gains)


def on_device(attn_heads, out_weight, residual, norm_gain):
    tensor = lax.axis_size("tensor")
    rows, block = residual.shape
    swap = [(0, 1), (1, 0)]

    def exchange(value, step):
        return lax.ppermute(value, "tensor", [(i, i ^ step) for i in range(tensor)])

    gain = norm_gain.reshape(-1, LANES)
    gain = jnp.pad(gain, ((0, -gain.shape[0] % 16), (0, 0)))
    relay = tensor == 4
    tiles = block // LANES
    half = tiles // 2
    parts = []
    spans = []
    gains = [gain] + [None] * (tensor - 1)

    def receive(part, first, last):
        parts.append(part)
        spans.append((first, last))
        return part

    def chip_products(steps, before=None, ready=None, after=()):
        rows_in = (own, peer)
        if before is not None:
            *rows_in, _ = lax.optimization_barrier((own, peer, before))
        keep, give, *later = project(*rows_in, ready, out_weight, tensor, steps, after)
        return keep, lax.ppermute(give, "seq", swap), *later

    peer = lax.ppermute(attn_heads, "seq", swap)
    far_steps = list(range(tensor - 1, tensor // 2 - 1, -1))
    near_steps = list(range(tensor // 2 - 1, 0, -1))
    own, ready = prefetch(attn_heads, out_weight, tensor, far_steps)
    keep, got, ready = chip_products(far_steps, None, ready, near_steps)
    keep_near, got_near = chip_products(near_steps, None, ready)
    if not relay:
        for wave, steps in enumerate((far_steps, near_steps)):
            plan = [(place, 0, tiles, True, BF16) for place in range(len(steps))]
            sums = pair_sum(plan, *((keep, got), (keep_near, got_near))[wave], gain)
            for step, value in zip(steps, sums):
                gains[step] = receive(exchange(value, step), 0, tiles)
        keep, got = chip_products([0], got_near)
        stream = finish_stream(keep, got, residual, parts, spans, 0, tiles)[0]
        pieces = [[stream]] + [[exchange(stream, step)] for step in range(1, tensor)]
        return normalize(pieces, gains, rows, block)
    plan = [
        (0, 0, half, False, BF16),
        (1, half, tiles, True, BF16),
        (0, half, tiles, True, BF16),
        (1, 0, half, False, F32),
    ]
    away, near, far, mine = pair_sum(plan, keep, got, gain)
    relayed = exchange(away, 1)
    gains[2] = receive(exchange(near, 2), half, tiles)
    gains[3] = receive(exchange(far, 3), half, tiles)
    beside = pair_sum([(0, 0, tiles, True, BF16)], keep_near, got_near, gain)[0]
    gains[1] = receive(exchange(beside, 1), 0, tiles)
    keep, got = chip_products([0], got_near)
    through = relay_sum(mine, relayed)
    last = exchange(through, 2)
    second = finish_stream(keep, got, residual, parts, spans, half, tiles)[0]
    relayed = exchange(second, 2)
    receive(last, 0, half)
    first, stream = finish_stream(keep, got, residual, parts, spans, 0, half, [second])
    beside = exchange(stream, 1)
    opposite = exchange(first, 2)
    direct = exchange(first, 3)
    through = exchange(relayed, 1)
    pieces = [[stream], [beside], [opposite, relayed], [direct, through]]
    return normalize(pieces, gains, rows, block)


def solution(mesh):
    in_specs = (
        P(("groups", "dp", "seq"), "tensor"),
        P(("tensor", "seq"), None),
        P(("groups", "dp", "seq"), "tensor"),
        P("tensor"),
    )
    out_specs = (P(("groups", "dp", "seq"), "tensor"), P(("groups", "dp", "seq"), None))

    return jax.shard_map(on_device, mesh=mesh, in_specs=in_specs, out_specs=out_specs, check_vma=False)
```

```python
import functools

import jax
import jax.numpy as jnp
from jax import lax
from jax.experimental import pallas as pl
from jax.experimental.pallas import tpu as pltpu
from jax.sharding import PartitionSpec as P


VMEM, HBM = pltpu.VMEM, pltpu.HBM
MIB = 1024 * 1024
F32, BF16 = jnp.float32, jnp.bfloat16
LANES = 128
READY = 2
LATER = 4
LAST = 1
HALF = 8
CHUNK = 512


def call(kernel, in_specs, out_shape, limit, scratch=(), out_space=VMEM):
    return pl.pallas_call(
        kernel,
        in_specs=[pl.BlockSpec(memory_space=space) for space in in_specs],
        out_specs=[pl.BlockSpec(memory_space=out_space)] * len(out_shape),
        out_shape=out_shape,
        scratch_shapes=list(scratch),
        compiler_params=pltpu.CompilerParams(vmem_limit_bytes=limit),
    )


def chunk_copies(tensor, chunk, steps, weight):
    block = weight.shape[1] // tensor
    rank = lax.axis_index("tensor")
    copies = []
    for step in steps:
        for piece in range(block // chunk):
            start = pl.multiple_of((rank ^ step) * block + piece * chunk, LANES)
            copies.append(functools.partial(pltpu.make_async_copy, weight.at[:, pl.ds(start, chunk)]))
    return copies


def prefetch_kernel(tensor, chunk, steps, own_hbm, weight, own_ref, ready_ref, own_sem, sems):
    depth = weight.shape[0]
    features = pl.ds(pl.multiple_of(lax.axis_index("seq") * depth, LANES), depth)
    own_copy = pltpu.make_async_copy(own_hbm.at[:, features], own_ref, own_sem)
    own_copy.start()
    copies = chunk_copies(tensor, chunk, steps, weight)[: ready_ref.shape[0]]
    copies = [copy(ready_ref.at[i], sems.at[i]) for i, copy in enumerate(copies)]
    for copy in copies:
        copy.start()
    for copy in copies:
        copy.wait()
    own_copy.wait()


def project_kernel(tensor, chunk, steps, early, after, own_ref, peer_ref, *refs):
    ready_refs, (weight, keep_ref, give_ref, *later_refs, held, sems, fence) = refs[:early], refs[early:]
    depth, width = weight.shape
    block = width // tensor
    per_block = block // chunk
    early = ready_refs[0].shape[0] if early else 0
    copies = chunk_copies(tensor, chunk, steps, weight)[early:]
    copies = [copy(held.at[i], sems.at[i]) for i, copy in enumerate(copies)]
    later = []
    if later_refs:
        later = chunk_copies(tensor, chunk, after, weight)[: later_refs[0].shape[0]]
        later = [copy(later_refs[0].at[i], sems.at[len(copies) + i]) for i, copy in enumerate(later)]
    for copy in copies + later:
        copy.start()
    pl.semaphore_signal(fence, 1)
    pl.semaphore_wait(fence, 1)
    features = pl.ds(pl.multiple_of(lax.axis_index("seq") * depth, LANES), depth)
    rows = own_ref.shape[0]
    operand = jnp.concatenate([own_ref[...], peer_ref[:, features]], axis=0)
    for index in range(len(steps) * per_block):
        place, piece = divmod(index, per_block)
        if index < early:
            right = ready_refs[0][index]
        else:
            copies[index - early].wait()
            right = held[index - early]
        product = jnp.dot(operand, right, preferred_element_type=F32)
        columns = pl.ds(piece * chunk, chunk)
        keep_ref[place, :, columns] = product[:rows]
        give_ref[place, :, columns] = product[rows:].astype(BF16)
    for copy in later:
        copy.wait()


def chunk_of(weight, tensor):
    block = weight.shape[1] // tensor
    chunk = min(block, CHUNK)
    return chunk, min(READY * MIB // (2 * weight.shape[0] * chunk), block // chunk)


def prefetch(own, weight, tensor, steps):
    rows, depth = own.shape[0], weight.shape[0]
    chunk, early = chunk_of(weight, tensor)
    return call(
        functools.partial(prefetch_kernel, tensor, chunk, steps),
        [HBM, HBM],
        [
            jax.ShapeDtypeStruct((rows, depth), BF16),
            jax.ShapeDtypeStruct((early, depth, chunk), BF16),
        ],
        2 * depth * chunk * early + 2 * MIB,
        [pltpu.SemaphoreType.DMA(()), pltpu.SemaphoreType.DMA((early,))],
    )(pltpu.with_memory_space_constraint(own, HBM), pltpu.with_memory_space_constraint(weight, HBM))


def project(own, peer, ready, weight, tensor, steps, after=()):
    rows = own.shape[0]
    depth, width = weight.shape
    block = width // tensor
    chunk, _ = chunk_of(weight, tensor)
    ready = [] if ready is None else [ready]
    early = ready[0].shape[0] if ready else 0
    count = len(steps) * block // chunk - early
    fetched = LATER if len(steps) > 1 else LAST
    later = min(fetched * MIB // (2 * depth * chunk), len(after) * block // chunk)
    shapes = [
        jax.ShapeDtypeStruct((len(steps), rows, block), F32),
        jax.ShapeDtypeStruct((len(steps), rows, block), BF16),
    ]
    if later:
        shapes.append(jax.ShapeDtypeStruct((later, depth, chunk), BF16))
    return call(
        functools.partial(project_kernel, tensor, chunk, steps, len(ready), after),
        [VMEM] * (2 + len(ready)) + [HBM],
        shapes,
        2 * depth * chunk * (len(steps) * block // chunk + later) + 4 * MIB,
        [VMEM((count, depth, chunk), BF16), pltpu.SemaphoreType.DMA((count + later,)), pltpu.SemaphoreType.REGULAR(())],
    )(own, peer, *ready, pltpu.with_memory_space_constraint(weight, HBM))


def pair_kernel(plan, keep_ref, got_ref, gain_ref, *out_refs):
    rows = keep_ref.shape[1]
    for (place, first, last, gained), target in zip(plan, out_refs):
        for tile in range(first, last):
            columns = slice(tile * LANES, (tile + 1) * LANES)
            value = keep_ref[place, :, columns] + got_ref[place, :, columns].astype(F32)
            target[(tile - first) * rows : (tile - first + 1) * rows, :] = value.astype(target.dtype)
        if gained:
            target[(last - first) * rows :, :] = gain_ref[...]


def pair_sum(plan, keep, got, gain):
    rows = keep.shape[1]
    shapes = [
        jax.ShapeDtypeStruct(((last - first) * rows + gained * gain.shape[0], LANES), dtype)
        for _, first, last, gained, dtype in plan
    ]
    kernel = functools.partial(pair_kernel, [entry[:4] for entry in plan])
    return call(kernel, [VMEM] * 3, shapes, 6 * MIB)(keep, got, gain)


def relay_kernel(mine_ref, got_ref, out_ref):
    out_ref[...] = (mine_ref[...] + got_ref[...].astype(F32)).astype(BF16)


def relay_sum(mine, got):
    shapes = [jax.ShapeDtypeStruct(mine.shape, BF16)]
    return call(relay_kernel, [VMEM] * 2, shapes, 4 * MIB)(mine, got)[0]


def stream_kernel(spans, first_tile, last_tile, early, keep_ref, got_ref, residual_ref, *refs):
    rows = keep_ref.shape[1]
    parts, refs = refs[: len(spans)], refs[len(spans) :]
    early_refs, (part_ref, *whole_refs) = refs[:early], refs[early:]
    for tile in range(first_tile, last_tile):
        columns = slice(tile * LANES, (tile + 1) * LANES)
        value = keep_ref[0, :, columns] + got_ref[0, :, columns].astype(F32)
        value = value + residual_ref[:, columns].astype(F32)
        for (first, last), part in zip(spans, parts):
            if first <= tile < last:
                value = value + part[(tile - first) * rows : (tile - first + 1) * rows, :].astype(F32)
        stream = value.astype(BF16)
        part_ref[(tile - first_tile) * rows : (tile - first_tile + 1) * rows, :] = stream
        for ref in whole_refs:
            ref[tile * rows : (tile + 1) * rows, :] = stream
    for early_ref, ref in zip(early_refs, whole_refs):
        ref[last_tile * rows :, :] = early_ref[...]


def finish_stream(keep, got, residual, parts, spans, first_tile, last_tile, early=()):
    _, rows, block = keep.shape
    shapes = [jax.ShapeDtypeStruct(((last_tile - first_tile) * rows, LANES), BF16)]
    shapes += [jax.ShapeDtypeStruct((rows * block // LANES, LANES), BF16)] * len(early)
    return call(
        functools.partial(stream_kernel, spans, first_tile, last_tile, len(early)),
        [VMEM] * (3 + len(parts) + len(early)),
        shapes,
        4 * MIB,
    )(keep, got, residual, *parts, *early)


def norm_kernel(rows, block, counts, gain_rows, *refs):
    tensor = len(counts)
    refs = list(refs)
    pieces = []
    for count in counts:
        group = [refs.pop(0) for _ in range(count)]
        pieces.append([(ref, tile) for ref in group for tile in range(ref.shape[0] // rows)])
    gains, (stream_hbm, out_hbm, stream_ref, out_ref, sems) = refs[:tensor], refs[tensor:]
    rank = lax.axis_index("tensor")
    copies = [pltpu.make_async_copy(stream_ref, stream_hbm, sems.at[tensor])]
    for step in range(tensor):
        start = pl.multiple_of((rank ^ step) * block, LANES)
        target = out_hbm.at[:, pl.ds(start, block)]
        copies.append(pltpu.make_async_copy(out_ref.at[step], target, sems.at[step]))
    for index, (ref, tile) in enumerate(pieces[0]):
        columns = slice(index * LANES, (index + 1) * LANES)
        stream_ref[:, columns] = ref[tile * rows : (tile + 1) * rows, :]
    copies[0].start()
    total = jnp.zeros((rows, LANES), F32)
    for piece in pieces:
        for ref, tile in piece:
            value = ref[tile * rows : (tile + 1) * rows, :].astype(F32)
            total = total + value * value
    mean_square = jnp.sum(total, axis=1, keepdims=True) / (tensor * block)
    scale = jnp.broadcast_to(lax.rsqrt(mean_square + 1e-05), (rows, LANES))
    for step, piece in enumerate(pieces):
        gain = gains[step][gains[step].shape[0] - gain_rows :, :].astype(F32)
        for index, (ref, tile) in enumerate(piece):
            value = ref[tile * rows : (tile + 1) * rows, :].astype(F32)
            scaled = value * scale * gain[index : index + 1, :]
            out_ref[step, :, index * LANES : (index + 1) * LANES] = scaled.astype(BF16)
        copies[step + 1].start()
    for copy in copies:
        copy.wait()


def normalize(pieces, gains, rows, block):
    tensor = len(gains)
    flat = [part for piece in pieces for part in piece]
    counts = [len(piece) for piece in pieces]
    return call(
        functools.partial(norm_kernel, rows, block, counts, gains[0].shape[0]),
        [VMEM] * (len(flat) + tensor),
        [
            jax.ShapeDtypeStruct((rows, block), BF16),
            jax.ShapeDtypeStruct((rows, tensor * block), BF16),
        ],
        6 * MIB,
        [
            VMEM((rows, block), BF16),
            VMEM((tensor, rows, block), BF16),
            pltpu.SemaphoreType.DMA((tensor + 1,)),
        ],
        HBM,
    )(*flat, *gains)


def on_device(attn_heads, out_weight, residual, norm_gain):
    tensor = lax.axis_size("tensor")
    rows, block = residual.shape
    swap = [(0, 1), (1, 0)]

    def exchange(value, step):
        return lax.ppermute(value, "tensor", [(i, i ^ step) for i in range(tensor)])

    gain = norm_gain.reshape(-1, LANES)
    gain = jnp.pad(gain, ((0, -gain.shape[0] % 16), (0, 0)))
    relay = tensor == 4
    tiles = block // LANES
    half = tiles * HALF // 16
    parts = []
    spans = []
    gains = [gain] + [None] * (tensor - 1)

    def receive(part, first, last):
        parts.append(part)
        spans.append((first, last))
        return part

    def chip_products(steps, before=None, ready=None, after=()):
        rows_in = (own, peer)
        if before is not None:
            *rows_in, _ = lax.optimization_barrier((own, peer, before))
        keep, give, *later = project(*rows_in, ready, out_weight, tensor, steps, after)
        return keep, lax.ppermute(give, "seq", swap), *later

    peer = lax.ppermute(attn_heads, "seq", swap)
    far_steps = list(range(tensor - 1, tensor // 2 - 1, -1))
    near_steps = list(range(tensor // 2 - 1, 0, -1))
    own, ready = prefetch(attn_heads, out_weight, tensor, far_steps)
    keep, got, ready = chip_products(far_steps, None, ready, near_steps)
    keep_near, got_near, *ready = chip_products(near_steps, None, ready, [0])
    ready = ready[0] if ready else None
    if not relay:
        for wave, steps in enumerate((far_steps, near_steps)):
            plan = [(place, 0, tiles, True, BF16) for place in range(len(steps))]
            sums = pair_sum(plan, *((keep, got), (keep_near, got_near))[wave], gain)
            for step, value in zip(steps, sums):
                gains[step] = receive(exchange(value, step), 0, tiles)
        keep, got = chip_products([0], got_near, ready)
        stream = finish_stream(keep, got, residual, parts, spans, 0, tiles)[0]
        pieces = [[stream]] + [[exchange(stream, step)] for step in range(1, tensor)]
        return normalize(pieces, gains, rows, block)
    plan = [
        (0, 0, half, False, BF16),
        (1, half, tiles, True, BF16),
        (0, half, tiles, True, BF16),
        (1, 0, half, False, F32),
    ]
    away, near, far, mine = pair_sum(plan, keep, got, gain)
    relayed = exchange(away, 1)
    gains[2] = receive(exchange(near, 2), half, tiles)
    gains[3] = receive(exchange(far, 3), half, tiles)
    beside = pair_sum([(0, 0, tiles, True, BF16)], keep_near, got_near, gain)[0]
    gains[1] = receive(exchange(beside, 1), 0, tiles)
    keep, got = chip_products([0], got_near, ready)
    through = relay_sum(mine, relayed)
    last = exchange(through, 2)
    second = finish_stream(keep, got, residual, parts, spans, half, tiles)[0]
    relayed = exchange(second, 2)
    receive(last, 0, half)
    first, stream = finish_stream(keep, got, residual, parts, spans, 0, half, [second])
    beside = exchange(stream, 1)
    opposite = exchange(first, 2)
    direct = exchange(first, 3)
    through = exchange(relayed, 1)
    pieces = [[stream], [beside], [opposite, relayed], [direct, through]]
    return normalize(pieces, gains, rows, block)


def solution(mesh):
    in_specs = (
        P(("groups", "dp", "seq"), "tensor"),
        P(("tensor", "seq"), None),
        P(("groups", "dp", "seq"), "tensor"),
        P("tensor"),
    )
    out_specs = (P(("groups", "dp", "seq"), "tensor"), P(("groups", "dp", "seq"), None))

    return jax.shard_map(on_device, mesh=mesh, in_specs=in_specs, out_specs=out_specs, check_vma=False)
```
